32 devices in a mesh: trial: 4 (over y, x), fsdp: 2 (over core), cols: 4 (over z).
Axes of the slice: x: 2, y: 2, z: 4, core: 2. Of those that a mesh axis runs over, the one named last changes fastest.
Arguments:
- train_gate: bfloat16 [8192, 8192], P(('trial', 'fsdp'), 'cols'), parts along dimension 0, may hold values from -0.1875 to 0.1875
- low_gate: bfloat16 [8192, 16], P(('trial', 'fsdp')), parts along dimension 0, may hold values from -0.125 to 0.125
- high_gate: bfloat16 [64, 8192], P('trial', 'cols'), parts along dimension 0, may hold values from -1.5 to 1.5
- train_up: bfloat16 [8192, 8192], P(('trial', 'fsdp'), 'cols'), parts along dimension 0, may hold values from -0.1875 to 0.1875
- low_up: bfloat16 [8192, 16], P(('trial', 'fsdp')), parts along dimension 0, may hold values from -0.125 to 0.125
- high_up: bfloat16 [64, 8192], P('trial', 'cols'), parts along dimension 0, may hold values from -1.5 to 1.5
- norm_gain: float32 [8192], P(('trial', 'fsdp')), parts along dimension 0, may hold values from 0.25 to 1.75
Outputs:
- ready_gate: bfloat16 [8192, 8192], P('trial', 'cols'), parts along dimension 0
- ready_up: bfloat16 [8192, 8192], P('trial', 'cols'), parts along dimension 0
- column_gate: float32 [32768], P(('trial', 'cols')), parts along dimension 0
- column_up: float32 [32768], P(('trial', 'cols')), parts along dimension 0
The draws below stay inside these ranges and needn't reach their ends.
There are 4 independent parts, one for each index of `trial`. The reference program is written for one: setup_inputs(seed, part) draws one part's arguments, and reference() takes and returns one part's arrays. A program takes and returns all parts, laid end to end along the dimension named above; each array names one. Nothing has to cross between parts.
All inputs are finite; a program needn't handle non-finite values. Where the reference program divides by a largest or mean magnitude, that divisor is 1e-20 or more.
Results may differ from the reference program's by a relative error of at most 0.001.
Values may be sent and summed in bfloat16 or wider, within the bound.
A program may use at most 128 MiB of HBM per device.

```python
import jax
import jax.numpy as jnp

D_MODEL = 2048
D_INNER = 8192
RANK = 16


def spiked(drawn, own_key, source, target, shards_of, factor):
    owner, partner = [(jnp.arange(drawn.shape[axis_at]) // (drawn.shape[axis_at] // shards_of)).reshape([-1 if axis == axis_at else 1 for axis in range(drawn.ndim)]) for axis_at in (source, target)]
    chosen = jax.random.permutation(own_key, shards_of)[partner]
    strong = (owner == chosen) | (owner == (partner + shards_of // 2) % shards_of)
    return jnp.where(strong, factor * drawn, drawn)


def levels(key, shape, split, least, high):
    def one(dim, parts):
        draws = jax.random.uniform(jax.random.fold_in(jax.random.fold_in(key, 6), dim), (parts,), jnp.float32, least / len(split), high / len(split))
        return jnp.repeat(jnp.exp(draws), shape[dim] // parts).reshape((-1,) + (1,) * (len(shape) - dim - 1))

    factor_of = one(*split[0])
    for cut in split[1:]:
        factor_of = factor_of * one(*cut)
    return factor_of


def gaussian(own_key, shape, spread, bound, shards=(), held_as=jnp.bfloat16):
    drawn = jax.random.normal(own_key, shape, jnp.float32) * spread
    if len(shards) > 0:
        drawn = levels(own_key, shape, shards, -0.22, 0.18) * drawn
    return jnp.clip(drawn, min=-bound, max=bound).astype(held_as)


def gaussian_with(stream_key, shape, spread, bound, split, heavy, kind=jnp.bfloat16):
    array = spread * jax.random.normal(stream_key, shape, jnp.float32)
    if split:
        array = array * levels(stream_key, shape, split, -0.22, 0.18)
    return jnp.clip(spiked(array, jax.random.fold_in(stream_key, 3), *heavy), -bound, bound).astype(kind)


def setup_inputs(seed: int = 0, part: int = 0) -> dict:
    seeds = jax.random.split(jax.random.key(seed), 8)
    own_keys = jax.random.split(jax.random.fold_in(seeds[7], part), 8)
    train_gate = gaussian_with(own_keys[0], (D_MODEL, D_INNER), D_MODEL ** -0.5, 0.1875, ((0, 2), (1, 4)), (0, 1, 4, 2.0))
    low_gate = gaussian(own_keys[1], (D_MODEL, RANK), D_MODEL ** -0.5, 0.125, ((0, 2),))
    high_gate = gaussian(own_keys[2], (RANK, D_INNER), RANK ** -0.5, 1.5, ((1, 4),))
    train_up = gaussian_with(own_keys[3], (D_MODEL, D_INNER), D_MODEL ** -0.5, 0.1875, ((0, 2), (1, 4)), (0, 1, 4, 2.0))
    low_up = gaussian(own_keys[4], (D_MODEL, RANK), D_MODEL ** -0.5, 0.125, ((0, 2),))
    high_up = gaussian(own_keys[5], (RANK, D_INNER), RANK ** -0.5, 1.5, ((1, 4),))
    norm_gain = jnp.clip(1.0 + 0.15 * jax.random.normal(own_keys[6], (D_MODEL,), jnp.float32), 0.25, 1.75)
    return {"train_gate": train_gate, "low_gate": low_gate, "high_gate": high_gate, "train_up": train_up, "low_up": low_up, "high_up": high_up, "norm_gain": norm_gain}


mix_rate = 1.0


def reference(train_gate, low_gate, high_gate, train_up, low_up, high_up, norm_gain):
    latest_gate = train_gate.astype(jnp.float32) + mix_rate * jnp.dot(low_gate, high_gate, preferred_element_type=jnp.float32)
    latest_up = train_up.astype(jnp.float32) + mix_rate * jnp.dot(low_up, high_up, preferred_element_type=jnp.float32)
    latest_gained_gate = latest_gate * norm_gain[:, None]
    latest_gained_up = latest_up * norm_gain[:, None]
    column_gate = jnp.max(jnp.abs(latest_gained_gate), axis=0)
    ready_gate = (latest_gained_gate / column_gate).astype(jnp.bfloat16)
    column_up = jnp.max(jnp.abs(latest_gained_up), axis=0)
    ready_up = (latest_gained_up / column_up).astype(jnp.bfloat16)
    return ready_gate, ready_up, column_gate, column_up
```

```python
import functools

import jax
import jax.numpy as jnp
from jax import lax
from jax.experimental import pallas as pl
from jax.experimental.pallas import tpu as pltpu
from jax.sharding import PartitionSpec as P

mix_rate = 1.0
STRIPE = 256
CHUNK = 128


def merge_kernel(parts, *refs):
    raws, lows, gains = refs[:parts], refs[parts : 2 * parts], refs[2 * parts : 3 * parts]
    high_ref, ready_ref, column_ref, gain_rows, gained = refs[3 * parts :]
    rows = raws[0].shape[0]
    width = high_ref.shape[1]
    chunk = min(CHUNK, rows)
    me = lax.axis_index("fsdp")

    @pl.when(pl.program_id(0) == 0)
    def _():
        for k in range(parts):
            spread = jnp.broadcast_to(gains[k][...], (128, rows))
            gain_rows[pl.ds(k * rows, rows), :] = spread.T

    high = high_ref[...]
    top = jnp.zeros((8, width), jnp.float32)
    for k in range(parts):
        for at in range(0, rows, chunk):
            low = lows[k][:, at : at + chunk]
            added = lax.dot_general(low, high, (((0,), (0,)), ((), ())), preferred_element_type=jnp.float32)
            latest = raws[k][at : at + chunk, :].astype(jnp.float32) + mix_rate * added
            gain = gain_rows[k * rows + at : k * rows + at + chunk, :]
            value = latest * jnp.concatenate([gain] * (width // 128), axis=1)
            gained[k * rows + at : k * rows + at + chunk, :] = value
            top = jnp.maximum(top, jnp.max(jnp.abs(value).reshape(chunk // 8, 8, width), axis=0))
    column = jnp.max(top, axis=0, keepdims=True)
    column_ref[...] = column
    scale = jnp.broadcast_to(1.0 / column, (8, width))
    for k in range(parts):
        owner = lax.rem(me - k + parts, parts)
        for at in range(0, rows, chunk):
            value = gained[k * rows + at : k * rows + at + chunk, :].reshape(chunk // 8, 8, width)
            scaled = (value * scale[None]).reshape(chunk, width).astype(jnp.bfloat16)
            start = pl.multiple_of(owner * rows + at, chunk)
            ready_ref[pl.ds(start, chunk), :] = scaled


def merge(raws, lows, gains, high):
    parts = len(raws)
    rows, columns = raws[0].shape
    rank = high.shape[0]
    stripe = min(STRIPE, columns)
    whole = lambda shape: pl.BlockSpec(shape, lambda j: (0, 0))
    ready, column = pl.pallas_call(
        functools.partial(merge_kernel, parts),
        grid=(columns // stripe,),
        out_shape=(
            jax.ShapeDtypeStruct((parts * rows, columns), jnp.bfloat16),
            jax.ShapeDtypeStruct((1, columns), jnp.float32),
        ),
        in_specs=[pl.BlockSpec((rows, stripe), lambda j: (0, j))] * parts
        + [whole((rank, rows))] * parts
        + [whole((1, rows))] * parts
        + [pl.BlockSpec((rank, stripe), lambda j: (0, j))],
        out_specs=(
            pl.BlockSpec((parts * rows, stripe), lambda j: (0, j)),
            pl.BlockSpec((1, stripe), lambda j: (0, j)),
        ),
        scratch_shapes=[
            pltpu.VMEM((parts * rows, 128), jnp.float32),
            pltpu.VMEM((parts * rows, stripe), jnp.float32),
        ],
        compiler_params=pltpu.CompilerParams(vmem_limit_bytes=24 * 1024 * 1024),
        cost_estimate=pl.CostEstimate(
            flops=16 * parts * rows * columns * rank, bytes_accessed=4 * parts * rows * columns, transcendentals=0
        ),
    )(*raws, *lows, *gains, high)
    return ready, column.reshape(columns)


def solution(mesh):
    parts = mesh.shape["fsdp"]

    def around(x):
        return [x] + [
            lax.ppermute(x, "fsdp", [(i, (i + k) % parts) for i in range(parts)]) for k in range(1, parts)
        ]

    def per_device(train_gate, low_gate, high_gate, train_up, low_up, high_up, norm_gain):
        gains = around(norm_gain.reshape(1, -1))
        low_gates = around(low_gate.T)
        low_ups = around(low_up.T)
        gates = around(train_gate)
        ups = around(train_up)
        ready_gate, column_gate = merge(gates, low_gates, gains, high_gate)
        ready_up, column_up = merge(ups, low_ups, gains, high_up)
        return ready_gate, ready_up, column_gate, column_up

    placed = (
        P(("trial", "fsdp"), "cols"),
        P(("trial", "fsdp"), None),
        P("trial", "cols"),
        P(("trial", "fsdp"), "cols"),
        P(("trial", "fsdp"), None),
        P("trial", "cols"),
        P(("trial", "fsdp")),
    )
    return jax.shard_map(
        per_device,
        mesh=mesh,
        in_specs=placed,
        out_specs=(
            P("trial", "cols"),
            P("trial", "cols"),
            P(("trial", "cols")),
            P(("trial", "cols")),
        ),
        check_vma=False,
    )
```

```python
import functools

import jax
import jax.numpy as jnp
from jax import lax
from jax.experimental import pallas as pl
from jax.experimental.pallas import tpu as pltpu
from jax.sharding import PartitionSpec as P


mix_rate = 1.0
STRIPE = 256
CHUNK = 128


def merge_kernel(parts, *refs):
    raws, lows, gains = refs[:parts], refs[parts : 2 * parts], refs[2 * parts : 3 * parts]
    high_ref, ready_ref, column_ref, gain_rows, low_rows, gained = refs[3 * parts :]
    rows = raws[0].shape[0]
    width = high_ref.shape[1]
    chunk = min(CHUNK, rows)
    me = lax.axis_index("fsdp")

    @pl.when(pl.program_id(0) == 0)
    def _():
        for k in range(parts):
            spread = jnp.broadcast_to(gains[k][...], (128, rows))
            gain_rows[pl.ds(k * rows, rows), :] = spread.T
            low_rows[pl.ds(k * rows, rows), :] = lows[k][...].astype(jnp.float32).T.astype(jnp.bfloat16)

    high = high_ref[...]
    top = jnp.zeros((8, width), jnp.float32)
    for k in range(parts):
        for at in range(0, rows, chunk):
            low = low_rows[k * rows + at : k * rows + at + chunk, :]
            added = jnp.dot(low, high, preferred_element_type=jnp.float32)
            latest = raws[k][at : at + chunk, :].astype(jnp.float32) + mix_rate * added
            gain = gain_rows[k * rows + at : k * rows + at + chunk, :]
            value = latest * jnp.concatenate([gain] * (width // 128), axis=1)
            gained[k * rows + at : k * rows + at + chunk, :] = value
            top = jnp.maximum(top, jnp.max(jnp.abs(value).reshape(chunk // 8, 8, width), axis=0))
    column = jnp.max(top, axis=0, keepdims=True)
    column_ref[...] = column
    scale = jnp.broadcast_to(1.0 / column, (8, width))
    for k in range(parts):
        owner = lax.rem(me - k + parts, parts)
        for at in range(0, rows, chunk):
            value = gained[k * rows + at : k * rows + at + chunk, :].reshape(chunk // 8, 8, width)
            scaled = (value * scale[None]).reshape(chunk, width).astype(jnp.bfloat16)
            start = pl.multiple_of(owner * rows + at, chunk)
            ready_ref[pl.ds(start, chunk), :] = scaled


def in_hbm(x):
    return pltpu.with_memory_space_constraint(x, pltpu.HBM)


def merge(raws, lows, gains, high):
    parts = len(raws)
    rows, columns = raws[0].shape
    rank = high.shape[0]
    stripe = min(STRIPE, columns)
    whole = lambda shape: pl.BlockSpec(shape, lambda j: (0, 0))
    ready, column = pl.pallas_call(
        functools.partial(merge_kernel, parts),
        grid=(columns // stripe,),
        out_shape=(
            jax.ShapeDtypeStruct((parts * rows, columns), jnp.bfloat16),
            jax.ShapeDtypeStruct((1, columns), jnp.float32),
        ),
        in_specs=[pl.BlockSpec((rows, stripe), lambda j: (0, j))] * parts
        + [whole((rank, rows))] * parts
        + [whole((1, rows))] * parts
        + [pl.BlockSpec((rank, stripe), lambda j: (0, j))],
        out_specs=(
            pl.BlockSpec((parts * rows, stripe), lambda j: (0, j)),
            pl.BlockSpec((1, stripe), lambda j: (0, j)),
        ),
        scratch_shapes=[
            pltpu.VMEM((parts * rows, 128), jnp.float32),
            pltpu.VMEM((parts * rows, rank), jnp.bfloat16),
            pltpu.VMEM((parts * rows, stripe), jnp.float32),
        ],
        compiler_params=pltpu.CompilerParams(vmem_limit_bytes=20 * 1024 * 1024),
        cost_estimate=pl.CostEstimate(
            flops=16 * parts * rows * columns * rank, bytes_accessed=4 * parts * rows * columns, transcendentals=0
        ),
    )(in_hbm(raws[0]), *raws[1:], in_hbm(lows[0]), *lows[1:], in_hbm(gains[0]), *gains[1:], in_hbm(high))
    return ready, column.reshape(columns)


def solution(mesh):
    parts = mesh.shape["fsdp"]

    def around(x):
        return [x] + [
            lax.ppermute(x, "fsdp", [(i, (i + k) % parts) for i in range(parts)]) for k in range(1, parts)
        ]

    def per_device(train_gate, low_gate, high_gate, train_up, low_up, high_up, norm_gain):
        gates = around(train_gate)
        low_gates = around(low_gate.T)
        gains = around(norm_gain.reshape(1, -1))
        low_ups = around(low_up.T)
        ups = around(train_up)
        ready_gate, column_gate = merge(gates, low_gates, gains, high_gate)
        ready_up, column_up = merge(ups, low_ups, gains, high_up)
        return ready_gate, ready_up, column_gate, column_up

    placed = (
        P(("trial", "fsdp"), "cols"),
        P(("trial", "fsdp"), None),
        P("trial", "cols"),
        P(("trial", "fsdp"), "cols"),
        P(("trial", "fsdp"), None),
        P("trial", "cols"),
        P(("trial", "fsdp")),
    )
    return jax.shard_map(
        per_device,
        mesh=mesh,
        in_specs=placed,
        out_specs=(
            P("trial", "cols"),
            P("trial", "cols"),
            P(("trial", "cols")),
            P(("trial", "cols")),
        ),
        check_vma=False,
    )
```

```python
import functools

import jax
import jax.numpy as jnp
from jax import lax
from jax.experimental import pallas as pl
from jax.experimental.pallas import tpu as pltpu
from jax.sharding import PartitionSpec as P


mix_rate = 1.0
STRIPE = 512
CHUNK = 128
BUDGET = 20 * 1024 * 1024


def spread(gain_ref, low_ref, gain_rows, low_rows, at):
    rows = gain_ref.shape[1]
    gain_rows[pl.ds(at, rows), :] = jnp.broadcast_to(gain_ref[...], (128, rows)).T
    low_rows[pl.ds(at, rows), :] = low_ref[...].astype(jnp.float32).T.astype(jnp.bfloat16)


def gained_rows(raw_ref, gain_rows, low_rows, high, out_ref, base, top):
    rows, width = raw_ref.shape
    chunk = min(CHUNK, rows)
    for at in range(0, rows, chunk):
        here = slice(base + at, base + at + chunk)
        added = jnp.dot(low_rows[here, :], high, preferred_element_type=jnp.float32)
        latest = raw_ref[at : at + chunk, :].astype(jnp.float32) + mix_rate * added
        value = latest * jnp.concatenate([gain_rows[here, :]] * (width // 128), axis=1)
        out_ref[here, :] = value
        top = jnp.maximum(top, jnp.max(jnp.abs(value).reshape(chunk // 8, 8, width), axis=0))
    return top


def own_kernel(raw_ref, low_ref, gain_ref, high_ref, value_ref, top_ref, gain_rows, low_rows):
    @pl.when(pl.program_id(0) == 0)
    def _():
        spread(gain_ref, low_ref, gain_rows, low_rows, 0)

    top = jnp.zeros(top_ref.shape, jnp.float32)
    top_ref[...] = gained_rows(raw_ref, gain_rows, low_rows, high_ref[...], value_ref, 0, top)


def merge_kernel(others, *refs):
    raws, lows, gains = refs[:others], refs[others : 2 * others], refs[2 * others : 3 * others]
    own_ref, top_ref, high_ref, ready_ref, column_ref, gain_rows, low_rows, gained = refs[3 * others :]
    rows, width = own_ref.shape
    chunk = min(CHUNK, rows)
    parts = others + 1
    me = lax.axis_index("fsdp")

    @pl.when(pl.program_id(0) == 0)
    def _():
        for k in range(others):
            spread(gains[k], lows[k], gain_rows, low_rows, k * rows)

    high = high_ref[...]
    top = top_ref[...]
    for k in range(others):
        top = gained_rows(raws[k], gain_rows, low_rows, high, gained, k * rows, top)
    column = jnp.max(top, axis=0, keepdims=True)
    column_ref[...] = column
    scale = jnp.broadcast_to(1.0 / column, (8, width))
    for k in range(parts):
        owner = lax.rem(me - k + parts, parts)
        for at in range(0, rows, chunk):
            value = own_ref[at : at + chunk, :] if k == 0 else gained[(k - 1) * rows + at : (k - 1) * rows + at + chunk, :]
            scaled = (value.reshape(chunk // 8, 8, width) * scale[None]).reshape(chunk, width).astype(jnp.bfloat16)
            ready_ref[pl.ds(pl.multiple_of(owner * rows + at, chunk), chunk), :] = scaled


def in_hbm(x):
    return pltpu.with_memory_space_constraint(x, pltpu.HBM)


def whole(shape):
    return pl.BlockSpec(shape, lambda j: (0, 0))


def striped(rows, stripe):
    return pl.BlockSpec((rows, stripe), lambda j: (0, j))


def cost(rows, columns, rank, ops):
    return pl.CostEstimate(flops=ops * rows * columns * rank, bytes_accessed=4 * rows * columns, transcendentals=0)


def own_part(raw, low, gain, high):
    rows, columns = raw.shape
    rank = high.shape[0]
    stripe = min(STRIPE, columns)
    return pl.pallas_call(
        own_kernel,
        grid=(columns // stripe,),
        out_shape=(
            jax.ShapeDtypeStruct((rows, columns), jnp.float32),
            jax.ShapeDtypeStruct((8, columns), jnp.float32),
        ),
        in_specs=[striped(rows, stripe), whole((rank, rows)), whole((1, rows)), striped(rank, stripe)],
        out_specs=(striped(rows, stripe), striped(8, stripe)),
        scratch_shapes=[pltpu.VMEM((rows, 128), jnp.float32), pltpu.VMEM((rows, rank), jnp.bfloat16)],
        compiler_params=pltpu.CompilerParams(vmem_limit_bytes=BUDGET),
        cost_estimate=cost(rows, columns, rank, 8),
    )(in_hbm(raw), in_hbm(low), in_hbm(gain), in_hbm(high))


def merge(own, raws, lows, gains, high):
    value, top = own
    others = len(raws)
    rows, columns = value.shape
    rank = high.shape[0]
    stripe = min(STRIPE, columns)
    ready, column = pl.pallas_call(
        functools.partial(merge_kernel, others),
        grid=(columns // stripe,),
        out_shape=(
            jax.ShapeDtypeStruct(((others + 1) * rows, columns), jnp.bfloat16),
            jax.ShapeDtypeStruct((1, columns), jnp.float32),
        ),
        in_specs=[striped(rows, stripe)] * others
        + [whole((rank, rows))] * others
        + [whole((1, rows))] * others
        + [striped(rows, stripe), striped(8, stripe), striped(rank, stripe)],
        out_specs=(striped((others + 1) * rows, stripe), striped(1, stripe)),
        scratch_shapes=[
            pltpu.VMEM((others * rows, 128), jnp.float32),
            pltpu.VMEM((others * rows, rank), jnp.bfloat16),
            pltpu.VMEM((others * rows, stripe), jnp.float32),
        ],
        compiler_params=pltpu.CompilerParams(vmem_limit_bytes=BUDGET),
        cost_estimate=cost(rows, columns, rank, 16 * (others + 1)),
    )(*raws, *lows, *gains, value, top, in_hbm(high))
    return ready, column.reshape(columns)


def whole_kernel(parts, *refs):
    raws, lows, gains = refs[:parts], refs[parts : 2 * parts], refs[2 * parts : 3 * parts]
    high_ref, ready_ref, column_ref, gain_rows, low_rows, gained = refs[3 * parts :]
    rows = raws[0].shape[0]
    width = high_ref.shape[1]
    chunk = min(CHUNK, rows)
    me = lax.axis_index("fsdp")

    @pl.when(pl.program_id(0) == 0)
    def _():
        for k in range(parts):
            spread = jnp.broadcast_to(gains[k][...], (128, rows))
            gain_rows[pl.ds(k * rows, rows), :] = spread.T
            low_rows[pl.ds(k * rows, rows), :] = lows[k][...].astype(jnp.float32).T.astype(jnp.bfloat16)

    high = high_ref[...]
    top = jnp.zeros((8, width), jnp.float32)
    for k in range(parts):
        for at in range(0, rows, chunk):
            low = low_rows[k * rows + at : k * rows + at + chunk, :]
            added = jnp.dot(low, high, preferred_element_type=jnp.float32)
            latest = raws[k][at : at + chunk, :].astype(jnp.float32) + mix_rate * added
            gain = gain_rows[k * rows + at : k * rows + at + chunk, :]
            value = latest * jnp.concatenate([gain] * (width // 128), axis=1)
            gained[k * rows + at : k * rows + at + chunk, :] = value
            top = jnp.maximum(top, jnp.max(jnp.abs(value).reshape(chunk // 8, 8, width), axis=0))
    column = jnp.max(top, axis=0, keepdims=True)
    column_ref[...] = column
    scale = jnp.broadcast_to(1.0 / column, (8, width))
    for k in range(parts):
        owner = lax.rem(me - k + parts, parts)
        for at in range(0, rows, chunk):
            value = gained[k * rows + at : k * rows + at + chunk, :].reshape(chunk // 8, 8, width)
            scaled = (value * scale[None]).reshape(chunk, width).astype(jnp.bfloat16)
            start = pl.multiple_of(owner * rows + at, chunk)
            ready_ref[pl.ds(start, chunk), :] = scaled


def merge_whole(raws, lows, gains, high):
    parts = len(raws)
    rows, columns = raws[0].shape
    rank = high.shape[0]
    stripe = min(STRIPE, columns)
    ready, column = pl.pallas_call(
        functools.partial(whole_kernel, parts),
        grid=(columns // stripe,),
        out_shape=(
            jax.ShapeDtypeStruct((parts * rows, columns), jnp.bfloat16),
            jax.ShapeDtypeStruct((1, columns), jnp.float32),
        ),
        in_specs=[pl.BlockSpec((rows, stripe), lambda j: (0, j))] * parts
        + [whole((rank, rows))] * parts
        + [whole((1, rows))] * parts
        + [pl.BlockSpec((rank, stripe), lambda j: (0, j))],
        out_specs=(
            pl.BlockSpec((parts * rows, stripe), lambda j: (0, j)),
            pl.BlockSpec((1, stripe), lambda j: (0, j)),
        ),
        scratch_shapes=[
            pltpu.VMEM((parts * rows, 128), jnp.float32),
            pltpu.VMEM((parts * rows, rank), jnp.bfloat16),
            pltpu.VMEM((parts * rows, stripe), jnp.float32),
        ],
        compiler_params=pltpu.CompilerParams(vmem_limit_bytes=BUDGET),
        cost_estimate=pl.CostEstimate(
            flops=16 * parts * rows * columns * rank, bytes_accessed=4 * parts * rows * columns, transcendentals=0
        ),
    )(in_hbm(raws[0]), *raws[1:], in_hbm(lows[0]), *lows[1:], in_hbm(gains[0]), *gains[1:], in_hbm(high))
    return ready, column.reshape(columns)


def solution(mesh):
    parts = mesh.shape["fsdp"]

    def around(x):
        return [lax.ppermute(x, "fsdp", [(i, (i + k) % parts) for i in range(parts)]) for k in range(1, parts)]

    def per_device(train_gate, low_gate, high_gate, train_up, low_up, high_up, norm_gain):
        gates = around(train_gate)
        low_gates = around(low_gate.T)
        gains = around(norm_gain.reshape(1, -1))
        low_ups = around(low_up.T)
        ups = around(train_up)
        own_gate = own_part(train_gate, low_gate.T, norm_gain.reshape(1, -1), high_gate)
        ready_gate, column_gate = merge(own_gate, gates, low_gates, gains, high_gate)
        ready_up, column_up = merge_whole([train_up] + ups, [low_up.T] + low_ups, [norm_gain.reshape(1, -1)] + gains, high_up)
        return ready_gate, ready_up, column_gate, column_up

    placed = (
        P(("trial", "fsdp"), "cols"),
        P(("trial", "fsdp"), None),
        P("trial", "cols"),
        P(("trial", "fsdp"), "cols"),
        P(("trial", "fsdp"), None),
        P("trial", "cols"),
        P(("trial", "fsdp")),
    )
    return jax.shard_map(
        per_device,
        mesh=mesh,
        in_specs=placed,
        out_specs=(
            P("trial", "cols"),
            P("trial", "cols"),
            P(("trial", "cols")),
            P(("trial", "cols")),
        ),
        check_vma=False,
    )
```
